16 devices in a mesh: dp: 1, sp: 16 (over x, y, z, core).
Axes of the slice: x: 2, y: 2, z: 2, core: 2. Of those that a mesh axis runs over, the one named last changes fastest.
Arguments:
- x: bfloat16 [2048, 8192], P(('dp', 'sp'))
- gain: bfloat16 [8192], replicated
- wq: bfloat16 [8192, 8192], replicated
- wk: bfloat16 [8192, 8192], replicated
- wv: bfloat16 [8192, 8192], replicated
- wo: bfloat16 [8192, 8192], replicated
Outputs:
- output: bfloat16 [2048, 8192], P(('dp', 'sp'))
All inputs are finite; a program needn't handle non-finite values.
Results may differ from the reference program's by a relative error of at most 0.012.
Values are sent between devices in bfloat16 or wider.
A program may use at most 2 GiB of HBM per device.

```python
import jax
import jax.numpy as jnp
from jax import lax

ROWS = 2048
D = 8192
HEADS = 64
KV_HEADS = 64
HEAD = 128
THETA = 10000


def setup_inputs(seed: int = 0, part: int = 0) -> dict:
    kx, kn, kq, kk, kv, ko = jax.random.split(jax.random.key(seed), 6)

    def weights(key, rows, columns):
        return jax.random.normal(key, (rows, columns), jnp.float32) * rows**-0.5

    drawn = {
        "x": jax.random.normal(jax.random.fold_in(kx, part), (ROWS, D), jnp.float32),
        "gain": 1 + 0.1 * jax.random.normal(kn, (D,), jnp.float32),
        "wq": 2 * weights(kq, D, HEADS * HEAD),
        "wk": 2 * weights(kk, D, KV_HEADS * HEAD),
        "wv": 4 * weights(kv, D, KV_HEADS * HEAD),
        "wo": weights(ko, HEADS * HEAD, D),
    }
    return {k: v.astype(jnp.bfloat16) for k, v in drawn.items()}


def normed(x, gain):
    wide = x.astype(jnp.float32)
    scale = lax.rsqrt(jnp.mean(wide * wide, -1, keepdims=True) + 1e-6)
    return (wide * scale * gain.astype(jnp.float32)).astype(jnp.bfloat16)


def turned(t, place, theta):
    half = t.shape[-1] // 2
    angle = place.astype(jnp.float32)[:, None] * theta ** (-jnp.arange(half, dtype=jnp.float32) / half)
    cos, sin = jnp.cos(angle)[:, None], jnp.sin(angle)[:, None]
    a, b = t[..., :half].astype(jnp.float32), t[..., half:].astype(jnp.float32)
    return jnp.concatenate([a * cos - b * sin, b * cos + a * sin], -1).astype(jnp.bfloat16)


def matmul(a, w):
    return jnp.dot(a, w, preferred_element_type=jnp.float32).astype(jnp.bfloat16)


def einsum(form, a, b):
    return jnp.einsum(form, a.astype(jnp.float32), b.astype(jnp.float32))


def attention(q, k, v):
    scores = einsum("tgsd,ugd->gstu", q, k) * q.shape[-1] ** -0.5
    token = jnp.arange(q.shape[0])
    scores = jnp.where(token[:, None] >= token, scores, -jnp.inf)
    weights = jax.nn.softmax(scores, -1).astype(jnp.bfloat16)
    return einsum("gstu,ugd->tgsd", weights, v).astype(jnp.bfloat16)


def reference(x, gain, wq, wk, wv, wo):
    a, place = normed(x, gain), jnp.arange(ROWS)
    q = turned(matmul(a, wq).reshape(ROWS, HEADS, HEAD), place, THETA).reshape(ROWS, KV_HEADS, -1, HEAD)
    k = turned(matmul(a, wk).reshape(ROWS, KV_HEADS, HEAD), place, THETA)
    v = matmul(a, wv).reshape(ROWS, KV_HEADS, HEAD)
    seen = attention(q, k, v).reshape(ROWS, HEADS * HEAD)
    return (x.astype(jnp.float32) + jnp.dot(seen, wo, preferred_element_type=jnp.float32)).astype(jnp.bfloat16)
```

```python
import functools

import jax
import jax.numpy as jnp
from jax import lax
from jax.experimental import pallas as pl
from jax.experimental.pallas import tpu as pltpu
from jax.sharding import PartitionSpec as P

HEAD = 128
THETA = 10000
LOG2E = 1.4426950408889634
NEG = -1e30
HIDDEN = 2 * NEG
PART = 256
WIDE = 256
RING = 6
SPAN = 512
MESH = pl.DeviceIdType.MESH


def _xor(a, b, bits):
    total = 0
    for n in range(bits):
        w = 2**n
        total += lax.rem(lax.rem(lax.div(a, w), 2) + lax.rem(lax.div(b, w), 2), 2) * w
    return total


def _dot(a, b, ca, cb):
    return lax.dot_general(a, b, (((ca,), (cb,)), ((), ())), preferred_element_type=jnp.float32)


def _kernel(x_hbm, gain, cos, sin, wq, wk, wv, wo, y_hbm,
            xall, a, ring, qs, ks, vs, qr, kr, vr, outs, seen, acc, top_s, mix_s,
            x_sem, ring_sem, send_sem, recv_sem, osend_sem, orecv_sem, dsend_sem, drecv_sem, ysend_sem, yrecv_sem, y_sem,
            *, chips):
    bits = chips.bit_length() - 1
    own = x_hbm.shape[0]
    tokens = 2 * own
    width = x_hbm.shape[1]
    half = width // 2
    groups = 2 * chips
    per = WIDE // HEAD
    me = lax.axis_index("sp")
    c, p = lax.div(me, 2), lax.rem(me, 2)
    partner = me + 1 - 2 * p

    def to(device):
        return dict(device_id={"sp": device}, device_id_type=MESH)

    barrier = pltpu.get_barrier_semaphore()
    pl.semaphore_signal(barrier, inc=1, **to(partner))
    for j in range(1, chips):
        pl.semaphore_signal(barrier, inc=1, **to(2 * _xor(c, j, bits) + p))

    def first_row(pair, chip):
        return pl.multiple_of((chip * 2 + pair) * WIDE, WIDE)

    def place(g):
        pair, jj = lax.div(g, chips), lax.rem(g, chips)
        return pair, jj, _xor(c, lax.rem(2 * chips - 1 - jj, chips), bits)

    def fetch(kind, g):
        pair, _, chip = place(g)
        at = pl.multiple_of(p * half + first_row(pair, chip), WIDE)
        slot = 3 * lax.rem(g, 2) + kind
        pltpu.make_async_copy((wq, wk, wv)[kind].at[:, :, :, pl.ds(at, WIDE)], ring.at[slot], ring_sem.at[slot]).start()

    def block_of(s):
        pair, jj = lax.div(s, chips), lax.rem(s, chips)
        j = lax.rem(chips - jj, chips)
        return pair, j, _xor(c, j, bits)

    def fetch_out(s):
        pair, _, chip = block_of(s)
        slot = lax.rem(s, RING)
        rows = pl.ds(first_row(pair, chip), WIDE)
        for n in range(half // WIDE):
            at = pl.multiple_of(p * half + n * WIDE, WIDE)
            pltpu.make_async_copy(wo.at[:, rows, pl.ds(at, WIDE)], ring.at[slot, n], ring_sem.at[slot]).start()

    def arrived(slot):
        pltpu.make_async_copy(ring.at[slot], ring.at[slot], ring_sem.at[slot]).wait()

    own_rows = pl.ds(pl.multiple_of(p * own, own), own)
    other_rows = pl.ds(pl.multiple_of((1 - p) * own, own), own)
    local = pltpu.make_async_copy(x_hbm, xall.at[own_rows], x_sem.at[0])
    local.start()
    for g in range(2):
        for kind in range(3):
            fetch(kind, g)
    pl.semaphore_wait(barrier, chips)
    across = pltpu.make_async_remote_copy(x_hbm, xall.at[own_rows], x_sem.at[1], x_sem.at[2], **to(partner))
    across.start()

    def norm(start):
        def rows(n, _):
            at = pl.ds(pl.multiple_of(start + n * 16, 16), 16)
            wide = xall[at, :].astype(jnp.float32)
            scale = lax.rsqrt(jnp.mean(wide * wide, -1, keepdims=True) + 1e-6)
            a[at, :] = (wide * scale * gain[...].astype(jnp.float32)).astype(jnp.bfloat16)

        lax.fori_loop(0, own // 16, rows, None)

    local.wait()
    norm(p * own)
    across.wait()
    norm((1 - p) * own)

    sends, recvs = (qs, ks, vs), (qr, kr, vr)

    def landing(kind, pair, chip):
        heads, rows = pl.ds(pair * per, per), pl.ds(pl.multiple_of(chip * tokens, tokens), tokens)
        return recvs[kind].at[heads, :, rows] if kind == 2 else recvs[kind].at[heads, rows, :]

    def parcel(kind, g):
        pair, jj, chip = place(g)
        return pltpu.make_async_remote_copy(
            sends[kind].at[g], landing(kind, pair, c), send_sem.at[kind, g], recv_sem.at[kind, g], **to(2 * chip + p))

    def far(g):
        return lax.rem(g, chips) < chips - 1

    def group(g, _):
        pair, jj, chip = place(g)
        for kind in range(3):
            slot = 3 * lax.rem(g, 2) + kind
            arrived(slot)
            got = jnp.dot(a[...], ring[slot].reshape(width, WIDE), preferred_element_type=jnp.float32)
            for h in range(per):
                t = got[:, h * HEAD : (h + 1) * HEAD].astype(jnp.bfloat16)
                if kind < 2:
                    t = t.astype(jnp.float32)
                    t = (t * cos[...] + pltpu.roll(t, HEAD // 2, 1) * sin[...]).astype(jnp.bfloat16)
                else:
                    t = t.T
                sends[kind][g, h] = t
                landing_here = t

                @pl.when(jj == chips - 1)
                def _():
                    rows = pl.ds(pl.multiple_of(c * tokens, tokens), tokens)
                    if kind == 2:
                        recvs[kind][pair * per + h, :, rows] = landing_here
                    else:
                        recvs[kind][pair * per + h, rows, :] = landing_here

            @pl.when(g + 2 < groups)
            def _():
                fetch(kind, g + 2)

            @pl.when(g + 2 >= groups)
            def _():
                fetch_out(3 * (g + 2 - groups) + kind)

            if kind:
                @pl.when(far(g))
                def _():
                    parcel(kind - 1, g).start()
            else:
                @pl.when((g > 0) & far(g + chips - 1))
                def _():
                    parcel(2, g - 1).start()

    lax.fori_loop(0, groups, group, None)

    def residual(n, _):
        rows = pl.ds(pl.multiple_of(n * 16, 16), 16)
        acc[rows, :] = xall[rows, pl.ds(pl.multiple_of(p * half, half), half)].astype(jnp.float32)

    lax.fori_loop(0, tokens // 16, residual, None)

    e = HEAD**-0.5 * LOG2E
    spans = chips * tokens // SPAN
    each = SPAN // tokens
    ones = jnp.ones((8, SPAN), jnp.bfloat16)

    def ship(pair, chip):
        j = _xor(c, chip, bits)
        return pltpu.make_async_remote_copy(
            outs.at[pair, chip], seen.at[pair * chips + c, p], osend_sem.at[pair, chip], orecv_sem.at[pair, j], **to(2 * chip + p))

    def span_of(m):
        return _xor(lax.div(c, each), spans - 1 - m, bits - 1)

    def ship_span(pair, m):
        for n in range(each):
            chip = span_of(m) * each + n

            @pl.when(chip != c)
            def _():
                ship(pair, chip).start()

    def attend(pair, _):
        def take(n, _):
            for kind in range(3):
                parcel(kind, pair * chips + n).wait_recv()

        lax.fori_loop(0, chips - 1, take, None)

        def span(m, _):
            at = span_of(m)
            mine = pl.ds(pl.multiple_of(at * SPAN, SPAN), SPAN)
            for h in range(per):
                top_s[h] = jnp.full((1, SPAN), NEG, jnp.float32)
                mix_s[h] = jnp.zeros((HEAD + 8, SPAN), jnp.float32)

            def block(j, masked):
                here = pl.ds(pl.multiple_of(j * SPAN, SPAN), SPAN)
                scores = [_dot(kr[pair * per + h, here, :], qr[pair * per + h, mine, :], 1, 1) for h in range(per)]
                weights, keeps = [], []
                for h, s in enumerate(scores):
                    if masked:
                        ok = lax.broadcasted_iota(jnp.int32, s.shape, 1) >= lax.broadcasted_iota(jnp.int32, s.shape, 0)
                        s = jnp.where(ok, s, HIDDEN)
                    old = top_s[h]
                    top = jnp.maximum(old, s.max(axis=0, keepdims=True))
                    top_s[h] = top
                    weights.append(jnp.exp2((s - top) * e).astype(jnp.bfloat16))
                    keeps.append(jnp.exp2((old - top) * e))
                for h, (w, keep) in enumerate(zip(weights, keeps)):
                    values = jnp.concatenate([vr[pair * per + h, :, here], ones], axis=0)
                    mix_s[h] = mix_s[h] * keep + _dot(values, w, 1, 0)

            lax.fori_loop(0, at, lambda j, _: block(j, False), None)
            block(at, True)
            for h in range(per):
                out = (mix_s[h, :HEAD, :] * (1 / mix_s[h, HEAD : HEAD + 1, :])).T.astype(jnp.bfloat16)
                for n in range(each):
                    chip = at * each + n
                    piece = out[n * tokens : (n + 1) * tokens]
                    outs[pair, chip, :, h * HEAD : (h + 1) * HEAD] = piece

                    @pl.when(chip == c)
                    def _():
                        seen[pair * chips + c, p, :, h * HEAD : (h + 1) * HEAD] = piece

            @pl.when(m > 0)
            def _():
                ship_span(pair, m - 1)

        lax.fori_loop(0, spans, span, None)
        ship_span(pair, spans - 1)

    lax.fori_loop(0, 2, attend, None)

    def hand(s):
        pair, _, chip = block_of(s)
        there = seen.at[pair * chips + chip, p]
        return pltpu.make_async_remote_copy(there, there, dsend_sem.at[s], drecv_sem.at[s], **to(partner))

    def take_in(s):
        pair, j, chip = block_of(s)

        @pl.when(j > 0)
        def _():
            ship(pair, chip).wait_recv()

        hand(s).start()

    take_in(0)

    def project(s, _):
        pair, _, chip = block_of(s)
        slot = lax.rem(s, RING)

        @pl.when(s + 1 < groups)
        def _():
            take_in(s + 1)

        arrived(slot)
        hand(s).wait_recv()
        left, right = seen[pair * chips + chip, 0], seen[pair * chips + chip, 1]
        for n in range(half // WIDE):
            cols = slice(n * WIDE, (n + 1) * WIDE)
            acc[:, cols] = acc[:, cols] + (
                jnp.dot(left, ring[slot, n, 0], preferred_element_type=jnp.float32)
                + jnp.dot(right, ring[slot, n, 1], preferred_element_type=jnp.float32))

        @pl.when(s + RING < groups)
        def _():
            fetch_out(s + RING)

    lax.fori_loop(0, groups, project, None)

    parts = 4
    size = half // parts

    def y_copies(n):
        cols = pl.ds(n * size, size)
        there = pl.ds(pl.multiple_of(p * half + n * size, size), size)
        return (pltpu.make_async_copy(a.at[own_rows, cols], y_hbm.at[:, there], y_sem.at[n]),
                pltpu.make_async_remote_copy(a.at[other_rows, cols], y_hbm.at[:, there], ysend_sem.at[n], yrecv_sem.at[n], **to(partner)))

    for n in range(parts + 1):
        if n < parts:
            cols = slice(n * size, (n + 1) * size)
            a[:, cols] = acc[:, cols].astype(jnp.bfloat16)
        if n:
            for copy in y_copies(n - 1):
                copy.start()

    def sent(n, _):
        hand(n).wait_send()

        @pl.when(far(n))
        def _():
            for kind in range(3):
                parcel(kind, n).wait_send()

        pair, chip = lax.div(n, chips), lax.rem(n, chips)

        @pl.when(chip != c)
        def _():
            ship(pair, chip).wait_send()

    lax.fori_loop(0, groups, sent, None)
    for n in range(parts):
        for copy in y_copies(n):
            copy.wait()


def solution(mesh):
    chips = mesh.shape["sp"] // 2

    def step(x, gain, wq, wk, wv, wo):
        own, width = x.shape
        tokens, half, groups = 2 * own, width // 2, 2 * chips
        place = lax.div(lax.axis_index("sp"), 2) * tokens + jnp.arange(tokens)
        angle = place.astype(jnp.float32)[:, None] * THETA ** (-jnp.arange(HEAD // 2, dtype=jnp.float32) / (HEAD // 2))
        cos, sin = jnp.cos(angle), jnp.sin(angle)
        cos, sin = jnp.concatenate([cos, cos], 1), jnp.concatenate([-sin, sin], 1)
        per = WIDE // HEAD
        low = jnp.bfloat16
        any_, vmem = pl.BlockSpec(memory_space=pl.ANY), pl.BlockSpec(memory_space=pltpu.VMEM)
        dma = pltpu.SemaphoreType.DMA
        whole = lambda w: w.reshape(width // (2 * PART), 2, PART, width)
        return pl.pallas_call(
            functools.partial(_kernel, chips=chips),
            out_shape=jax.ShapeDtypeStruct((own, width), low),
            in_specs=[any_, vmem, vmem, vmem, any_, any_, any_, any_],
            out_specs=any_,
            scratch_shapes=[
                pltpu.VMEM((tokens, width), low),
                pltpu.VMEM((tokens, width), low),
                pltpu.VMEM((RING, width // (2 * PART), 2, PART, WIDE), low),
                pltpu.VMEM((groups, per, tokens, HEAD), low),
                pltpu.VMEM((groups, per, tokens, HEAD), low),
                pltpu.VMEM((groups, per, HEAD, tokens), low),
                pltpu.VMEM((2 * per, chips * tokens, HEAD), low),
                pltpu.VMEM((2 * per, chips * tokens, HEAD), low),
                pltpu.VMEM((2 * per, HEAD, chips * tokens), low),
                pltpu.VMEM((2, chips, tokens, WIDE), low),
                pltpu.VMEM((groups, 2, tokens, WIDE), low),
                pltpu.VMEM((tokens, half), jnp.float32),
                pltpu.VMEM((per, 1, SPAN), jnp.float32),
                pltpu.VMEM((per, HEAD + 8, SPAN), jnp.float32),
                dma((3,)), dma((RING,)), dma((3, groups)), dma((3, groups)), dma((2, chips)), dma((2, chips)),
                dma((groups,)), dma((groups,)), dma((4,)), dma((4,)), dma((4,)),
            ],
            compiler_params=pltpu.CompilerParams(collective_id=0, has_side_effects=True, vmem_limit_bytes=63 * 2**20),
        )(x, gain[None], cos, sin, whole(wq), whole(wk), whole(wv), wo.reshape(2, half, width))

    tokens, whole = P(("dp", "sp"), None), P(None, None)
    return jax.shard_map(
        step,
        mesh=mesh,
        in_specs=(tokens, P(None), whole, whole, whole, whole),
        out_specs=tokens,
        check_vma=False,
    )
```

```python
import functools

import jax
import jax.numpy as jnp
from jax import lax
from jax.experimental import pallas as pl
from jax.experimental.pallas import tpu as pltpu
from jax.sharding import PartitionSpec as P

HEAD = 128
THETA = 10000
LOG2E = 1.4426950408889634
NEG = -1e30
HIDDEN = 2 * NEG
PART = 256
WIDE = 256
TILE = 128
RING = 6
SPAN = 512
SEND = (7, 6, 1, 5, 2, 3, 4, 0)
SPANS = (3, 0, 2, 1)
TAKE = (0, 7, 6, 1, 5, 4, 3, 2)
MESH = pl.DeviceIdType.MESH


def _xor(a, b, bits):
    total = 0
    for n in range(bits):
        w = 2**n
        total += lax.rem(lax.rem(lax.div(a, w), 2) + lax.rem(lax.div(b, w), 2), 2) * w
    return total


def _pick(n, values):
    got = values[-1]
    for i in range(len(values) - 1):
        got = jnp.where(n == i, values[i], got)
    return got


def _dot(a, b, ca, cb):
    return lax.dot_general(a, b, (((ca,), (cb,)), ((), ())), preferred_element_type=jnp.float32)


def _kernel(x_hbm, gain, cos, sin, wq, wk, wv, wo, y_hbm,
            xall, a, ring, qs, ks, vs, qr, kr, vr, outs, seen, acc, top_s, mix_s,
            x_sem, ring_sem, send_sem, recv_sem, osend_sem, orecv_sem, dsend_sem, drecv_sem, ysend_sem, yrecv_sem, y_sem,
            *, chips):
    bits = chips.bit_length() - 1
    own = x_hbm.shape[0]
    tokens = 2 * own
    width = x_hbm.shape[1]
    half = width // 2
    groups = 2 * chips
    per = WIDE // HEAD
    me = lax.axis_index("sp")
    c, p = lax.div(me, 2), lax.rem(me, 2)
    partner = me + 1 - 2 * p

    def to(device):
        return dict(device_id={"sp": device}, device_id_type=MESH)

    barrier = pltpu.get_barrier_semaphore()
    pl.semaphore_signal(barrier, inc=1, **to(partner))
    for j in range(1, chips):
        pl.semaphore_signal(barrier, inc=1, **to(2 * _xor(c, j, bits) + p))

    def first_row(pair, chip):
        return pl.multiple_of((chip * 2 + pair) * WIDE, WIDE)

    def place(g):
        pair, jj = lax.div(g, chips), lax.rem(g, chips)
        return pair, jj, _xor(c, _pick(jj, SEND), bits)

    def fetch(kind, g):
        pair, _, chip = place(g)
        at = pl.multiple_of(p * half + first_row(pair, chip), WIDE)
        slot = 3 * lax.rem(g, 2) + kind
        for n in range(WIDE // TILE):
            cols = pl.ds(pl.multiple_of(at + n * TILE, TILE), TILE)
            pltpu.make_async_copy((wq, wk, wv)[kind].at[:, :, :, cols], ring.at[slot, n], ring_sem.at[slot]).start()

    def block_of(s):
        pair, jj = lax.div(s, chips), lax.rem(s, chips)
        j = _pick(jj, TAKE)
        return pair, j, _xor(c, j, bits)

    def fetch_out(s):
        pair, _, chip = block_of(s)
        slot = lax.rem(s, RING)
        rows = pl.ds(first_row(pair, chip), WIDE)
        for n in range(half // TILE):
            at = pl.multiple_of(p * half + n * TILE, TILE)
            pltpu.make_async_copy(wo.at[:, rows, pl.ds(at, TILE)], ring.at[slot, *divmod(n, half // WIDE)], ring_sem.at[slot]).start()

    def arrived(slot):
        pltpu.make_async_copy(ring.at[slot], ring.at[slot], ring_sem.at[slot]).wait()

    own_rows = pl.ds(pl.multiple_of(p * own, own), own)
    other_rows = pl.ds(pl.multiple_of((1 - p) * own, own), own)
    local = pltpu.make_async_copy(x_hbm, xall.at[own_rows], x_sem.at[0])
    local.start()
    for g in range(2):
        for kind in range(3):
            fetch(kind, jnp.int32(g))
    pl.semaphore_wait(barrier, chips)
    across = pltpu.make_async_remote_copy(x_hbm, xall.at[own_rows], x_sem.at[1], x_sem.at[2], **to(partner))
    across.start()

    tiles = width // TILE
    band = 32

    def norm(start):
        def rows(n, _):
            at = pl.ds(pl.multiple_of(start + n * band, band), band)
            total = jnp.zeros((band, TILE), jnp.float32)
            for t in range(tiles):
                wide = xall[at, t * TILE : (t + 1) * TILE].astype(jnp.float32)
                total += wide * wide
            scale = lax.rsqrt(jnp.sum(total, -1, keepdims=True) * (1 / width) + 1e-6)
            for t in range(tiles):
                wide = xall[at, t * TILE : (t + 1) * TILE].astype(jnp.float32)
                a[t, at, :] = (wide * scale * gain[:, t * TILE : (t + 1) * TILE].astype(jnp.float32)).astype(jnp.bfloat16)

        lax.fori_loop(0, own // band, rows, None)

    local.wait()
    norm(p * own)
    across.wait()
    norm((1 - p) * own)

    sends, recvs = (qs, ks, vs), (qr, kr, vr)

    def landing(kind, pair, chip):
        heads, rows = pl.ds(pair * per, per), pl.ds(pl.multiple_of(chip * tokens, tokens), tokens)
        return recvs[kind].at[heads, :, rows] if kind == 2 else recvs[kind].at[heads, rows, :]

    def parcel(kind, g):
        pair, jj, chip = place(g)
        return pltpu.make_async_remote_copy(
            sends[kind].at[g], landing(kind, pair, c), send_sem.at[kind, g], recv_sem.at[kind, g], **to(2 * chip + p))

    def far(g):
        return lax.rem(g, chips) < chips - 1

    def group(g, _):
        pair, jj, chip = place(g)
        for kind in range(3):
            slot = 3 * lax.rem(g, 2) + kind
            arrived(slot)
            left = jnp.concatenate([a[t] for t in range(tiles)], 1)
            right = jnp.concatenate([ring[slot, n].reshape(width, TILE) for n in range(WIDE // TILE)], 1)
            got = jnp.dot(left, right, preferred_element_type=jnp.float32)
            for h in range(per):
                t = got[:, h * HEAD : (h + 1) * HEAD].astype(jnp.bfloat16)
                if kind < 2:
                    t = t.astype(jnp.float32)
                    t = (t * cos[...] + pltpu.roll(t, HEAD // 2, 1) * sin[...]).astype(jnp.bfloat16)
                else:
                    t = t.T
                sends[kind][g, h] = t
                rows = pl.ds(pl.multiple_of(c * tokens, tokens), tokens)
                if kind == 2:
                    recvs[kind][pair * per + h, :, rows] = t
                else:
                    recvs[kind][pair * per + h, rows, :] = t

            @pl.when(g + 2 < groups)
            def _():
                fetch(kind, g + 2)

            @pl.when(g + 2 >= groups)
            def _():
                fetch_out(3 * (g + 2 - groups) + kind)

            if kind:
                @pl.when(far(g))
                def _():
                    parcel(kind - 1, g).start()
            else:
                @pl.when((g > 0) & far(g + chips - 1))
                def _():
                    parcel(2, g - 1).start()

    lax.fori_loop(0, groups, group, None)

    def residual(n, _):
        rows = pl.ds(pl.multiple_of(n * 16, 16), 16)
        acc[rows, :] = xall[rows, pl.ds(pl.multiple_of(p * half, half), half)].astype(jnp.float32)

    lax.fori_loop(0, tokens // 16, residual, None)

    e = HEAD**-0.5 * LOG2E
    spans = chips * tokens // SPAN
    each = SPAN // tokens
    ones = jnp.ones((8, SPAN), jnp.bfloat16)

    def ship(pair, chip):
        j = _xor(c, chip, bits)
        return pltpu.make_async_remote_copy(
            outs.at[pair, chip], seen.at[pair * chips + c, p], osend_sem.at[pair, chip], orecv_sem.at[pair, j], **to(2 * chip + p))

    def span_of(m):
        return _xor(lax.div(c, each), _pick(m, SPANS), bits - 1)

    def ship_span(pair, m):
        for n in range(each):
            chip = span_of(m) * each + n

            @pl.when(chip != c)
            def _():
                ship(pair, chip).start()

    def attend(pair, _):
        def take(n, _):
            for kind in range(3):
                parcel(kind, pair * chips + n).wait_recv()

        lax.fori_loop(0, chips - 1, take, None)

        def span(m, _):
            at = span_of(m)
            mine = pl.ds(pl.multiple_of(at * SPAN, SPAN), SPAN)
            for h in range(per):
                top_s[h] = jnp.full((1, SPAN), NEG, jnp.float32)
                mix_s[h] = jnp.zeros((HEAD + 8, SPAN), jnp.float32)

            def block(j, masked):
                here = pl.ds(pl.multiple_of(j * SPAN, SPAN), SPAN)
                scores = [_dot(kr[pair * per + h, here, :], qr[pair * per + h, mine, :], 1, 1) for h in range(per)]
                weights, keeps = [], []
                for h, s in enumerate(scores):
                    if masked:
                        ok = lax.broadcasted_iota(jnp.int32, s.shape, 1) >= lax.broadcasted_iota(jnp.int32, s.shape, 0)
                        s = jnp.where(ok, s, HIDDEN)
                    old = top_s[h]
                    top = jnp.maximum(old, s.max(axis=0, keepdims=True))
                    top_s[h] = top
                    weights.append(jnp.exp2((s - top) * e).astype(jnp.bfloat16))
                    keeps.append(jnp.exp2((old - top) * e))
                for h, (w, keep) in enumerate(zip(weights, keeps)):
                    values = jnp.concatenate([vr[pair * per + h, :, here], ones], axis=0)
                    mix_s[h] = mix_s[h] * keep + _dot(values, w, 1, 0)

            lax.fori_loop(0, at, lambda j, _: block(j, False), None)
            block(at, True)
            for h in range(per):
                out = (mix_s[h, :HEAD, :] * (1 / mix_s[h, HEAD : HEAD + 1, :])).T.astype(jnp.bfloat16)
                for n in range(each):
                    chip = at * each + n
                    piece = out[n * tokens : (n + 1) * tokens]
                    outs[pair, chip, h] = piece
                    seen[jnp.where(chip == c, pair * chips + c, groups), p, h] = piece

            @pl.when(m > 0)
            def _():
                ship_span(pair, m - 1)

        lax.fori_loop(0, spans, span, None)
        ship_span(pair, jnp.int32(spans - 1))

    lax.fori_loop(0, 2, attend, None)

    def hand(s):
        pair, _, chip = block_of(s)
        there = seen.at[pair * chips + chip, p]
        return pltpu.make_async_remote_copy(there, there, dsend_sem.at[s], drecv_sem.at[s], **to(partner))

    def take_in(s):
        pair, j, chip = block_of(s)

        @pl.when(j > 0)
        def _():
            ship(pair, chip).wait_recv()

        hand(s).start()

    take_in(jnp.int32(0))

    def project(s, _):
        pair, _, chip = block_of(s)
        slot = lax.rem(s, RING)

        @pl.when(s + 1 < groups)
        def _():
            take_in(s + 1)

        arrived(slot)
        hand(s).wait_recv()
        left = jnp.concatenate([seen[pair * chips + chip, i, h] for i in range(2) for h in range(per)], 1)
        for n in range(half // WIDE):
            cols = slice(n * WIDE, (n + 1) * WIDE)
            slabs = [divmod(n * (WIDE // TILE) + i, half // WIDE) for i in range(WIDE // TILE)]
            right = jnp.concatenate([ring[slot, i, j].reshape(2 * PART, TILE) for i, j in slabs], 1)
            acc[:, cols] += jnp.dot(left, right, preferred_element_type=jnp.float32)

        @pl.when(s + RING < groups)
        def _():
            fetch_out(s + RING)

    lax.fori_loop(0, groups, project, None)

    parts = 4
    size = half // parts

    def y_copies(n):
        cols = pl.ds(n * size, size)
        there = pl.ds(pl.multiple_of(p * half + n * size, size), size)
        return (pltpu.make_async_copy(xall.at[own_rows, cols], y_hbm.at[:, there], y_sem.at[n]),
                pltpu.make_async_remote_copy(xall.at[other_rows, cols], y_hbm.at[:, there], ysend_sem.at[n], yrecv_sem.at[n], **to(partner)))

    for n in range(parts + 1):
        if n < parts:
            cols = slice(n * size, (n + 1) * size)
            xall[:, cols] = acc[:, cols].astype(jnp.bfloat16)
        if n:
            for copy in y_copies(n - 1):
                copy.start()

    def sent(n, _):
        hand(n).wait_send()

        @pl.when(far(n))
        def _():
            for kind in range(3):
                parcel(kind, n).wait_send()

        pair, chip = lax.div(n, chips), lax.rem(n, chips)

        @pl.when(chip != c)
        def _():
            ship(pair, chip).wait_send()

    lax.fori_loop(0, groups, sent, None)
    for n in range(parts):
        for copy in y_copies(n):
            copy.wait()


def solution(mesh):
    chips = mesh.shape["sp"] // 2

    def step(x, gain, wq, wk, wv, wo):
        own, width = x.shape
        tokens, half, groups = 2 * own, width // 2, 2 * chips
        place = lax.div(lax.axis_index("sp"), 2) * tokens + jnp.arange(tokens)
        angle = place.astype(jnp.float32)[:, None] * THETA ** (-jnp.arange(HEAD // 2, dtype=jnp.float32) / (HEAD // 2))
        cos, sin = jnp.cos(angle), jnp.sin(angle)
        cos, sin = jnp.concatenate([cos, cos], 1), jnp.concatenate([-sin, sin], 1)
        per = WIDE // HEAD
        low = jnp.bfloat16
        any_, vmem = pl.BlockSpec(memory_space=pl.ANY), pl.BlockSpec(memory_space=pltpu.VMEM)
        dma = pltpu.SemaphoreType.DMA
        whole = lambda w: w.reshape(width // (2 * PART), 2, PART, width)
        return pl.pallas_call(
            functools.partial(_kernel, chips=chips),
            out_shape=jax.ShapeDtypeStruct((own, width), low),
            in_specs=[any_, vmem, vmem, vmem, any_, any_, any_, any_],
            out_specs=any_,
            scratch_shapes=[
                pltpu.VMEM((tokens, width), low),
                pltpu.VMEM((width // TILE, tokens, TILE), low),
                pltpu.VMEM((RING, WIDE // TILE, width // (2 * PART), 2, PART, TILE), low),
                pltpu.VMEM((groups, per, tokens, HEAD), low),
                pltpu.VMEM((groups, per, tokens, HEAD), low),
                pltpu.VMEM((groups, per, HEAD, tokens), low),
                pltpu.VMEM((2 * per, chips * tokens, HEAD), low),
                pltpu.VMEM((2 * per, chips * tokens, HEAD), low),
                pltpu.VMEM((2 * per, HEAD, chips * tokens), low),
                pltpu.VMEM((2, chips, per, tokens, HEAD), low),
                pltpu.VMEM((groups + 1, 2, per, tokens, HEAD), low),
                pltpu.VMEM((tokens, half), jnp.float32),
                pltpu.VMEM((per, 1, SPAN), jnp.float32),
                pltpu.VMEM((per, HEAD + 8, SPAN), jnp.float32),
                dma((3,)), dma((RING,)), dma((3, groups)), dma((3, groups)), dma((2, chips)), dma((2, chips)),
                dma((groups,)), dma((groups,)), dma((4,)), dma((4,)), dma((4,)),
            ],
            compiler_params=pltpu.CompilerParams(collective_id=0, has_side_effects=True, vmem_limit_bytes=63 * 2**20),
        )(x, gain[None], cos, sin, whole(wq), whole(wk), whole(wv), wo.reshape(2, half, width))

    tokens, whole = P(("dp", "sp"), None), P(None, None)
    return jax.shard_map(
        step,
        mesh=mesh,
        in_specs=(tokens, P(None), whole, whole, whole, whole),
        out_specs=tokens,
        check_vma=False,
    )
```

```python
import functools

import jax
import jax.numpy as jnp
from jax import lax
from jax.experimental import pallas as pl
from jax.experimental.pallas import tpu as pltpu
from jax.sharding import PartitionSpec as P

HEAD = 128
THETA = 10000
LOG2E = 1.4426950408889634
NEG = -1e30
HIDDEN = 2 * NEG
PART = 256
WIDE = 256
TILE = 128
RING = 6
SPAN = 512
SEND = (7, 6, 1, 5, 2, 3, 4, 0)
SPANS = (3, 0, 2, 1)
TAKE = (0, 7, 6, 1, 5, 4, 3, 2)
MESH = pl.DeviceIdType.MESH


def _xor(a, b, bits):
    total = 0
    for n in range(bits):
        w = 2**n
        total += lax.rem(lax.rem(lax.div(a, w), 2) + lax.rem(lax.div(b, w), 2), 2) * w
    return total


def _pick(n, values):
    got = values[-1]
    for i in range(len(values) - 1):
        got = jnp.where(n == i, values[i], got)
    return got


def _dot(a, b, ca, cb):
    return lax.dot_general(a, b, (((ca,), (cb,)), ((), ())), preferred_element_type=jnp.float32)


def _kernel(x_hbm, gain, cos, sin, wq, wk, wv, wo, y_hbm,
            xall, a, ring, made, got, turned_v, outs, seen, acc, top_s, mix_s,
            x_sem, ring_sem, send_sem, recv_sem, osend_sem, orecv_sem, dsend_sem, drecv_sem, ysend_sem, yrecv_sem, y_sem,
            *, chips):
    bits = chips.bit_length() - 1
    own = x_hbm.shape[0]
    tokens = 2 * own
    width = x_hbm.shape[1]
    half = width // 2
    groups = 2 * chips
    per = WIDE // HEAD
    me = lax.axis_index("sp")
    c, p = lax.div(me, 2), lax.rem(me, 2)
    partner = me + 1 - 2 * p

    def to(device):
        return dict(device_id={"sp": device}, device_id_type=MESH)

    barrier = pltpu.get_barrier_semaphore()
    pl.semaphore_signal(barrier, inc=1, **to(partner))
    for j in range(1, chips):
        pl.semaphore_signal(barrier, inc=1, **to(2 * _xor(c, j, bits) + p))

    def first_row(pair, chip):
        return pl.multiple_of((chip * 2 + pair) * WIDE, WIDE)

    def place(g):
        pair, jj = lax.div(g, chips), lax.rem(g, chips)
        return pair, jj, _xor(c, _pick(jj, SEND), bits)

    def fetch(t):
        kind, g = lax.rem(t, 3), lax.div(t, 3)
        pair, _, chip = place(g)
        at = pl.multiple_of(p * half + first_row(pair, chip), WIDE)
        slot = lax.rem(t, RING)
        for k, w in enumerate((wq, wk, wv)):
            @pl.when(kind == k)
            def _():
                for n in range(WIDE // TILE):
                    cols = pl.ds(pl.multiple_of(at + n * TILE, TILE), TILE)
                    pltpu.make_async_copy(w.at[:, :, :, cols], ring.at[slot, n], ring_sem.at[slot]).start()

    def block_of(s):
        pair, jj = lax.div(s, chips), lax.rem(s, chips)
        j = _pick(jj, TAKE)
        return pair, j, _xor(c, j, bits)

    def fetch_out(s):
        pair, _, chip = block_of(s)
        slot = lax.rem(s, RING)
        rows = pl.ds(first_row(pair, chip), WIDE)
        for n in range(half // TILE):
            at = pl.multiple_of(p * half + n * TILE, TILE)
            pltpu.make_async_copy(wo.at[:, rows, pl.ds(at, TILE)], ring.at[slot, *divmod(n, half // WIDE)], ring_sem.at[slot]).start()

    def arrived(slot):
        pltpu.make_async_copy(ring.at[slot], ring.at[slot], ring_sem.at[slot]).wait()

    own_rows = pl.ds(pl.multiple_of(p * own, own), own)
    other_rows = pl.ds(pl.multiple_of((1 - p) * own, own), own)
    local = pltpu.make_async_copy(x_hbm, xall.at[own_rows], x_sem.at[0])
    local.start()
    for t in range(RING):
        fetch(jnp.int32(t))
    pl.semaphore_wait(barrier, chips)
    across = pltpu.make_async_remote_copy(x_hbm, xall.at[own_rows], x_sem.at[1], x_sem.at[2], **to(partner))
    across.start()

    tiles = width // TILE
    band = 32

    def norm(start):
        def rows(n, _):
            at = pl.ds(pl.multiple_of(start + n * band, band), band)
            total = jnp.zeros((band, TILE), jnp.float32)
            for t in range(tiles):
                wide = xall[at, t * TILE : (t + 1) * TILE].astype(jnp.float32)
                total += wide * wide
            scale = lax.rsqrt(jnp.sum(total, -1, keepdims=True) * (1 / width) + 1e-6)
            for t in range(tiles):
                wide = xall[at, t * TILE : (t + 1) * TILE].astype(jnp.float32)
                a[t, at, :] = (wide * scale * gain[:, t * TILE : (t + 1) * TILE].astype(jnp.float32)).astype(jnp.bfloat16)

        lax.fori_loop(0, own // band, rows, None)

    local.wait()
    norm(p * own)
    across.wait()
    norm((1 - p) * own)

    def parcel(t):
        kind, g = lax.rem(t, 3), lax.div(t, 3)
        pair, _, chip = place(g)
        there = got.at[kind, pl.ds(pair * per, per), pl.ds(pl.multiple_of(c * tokens, tokens), tokens), :]
        return pltpu.make_async_remote_copy(made.at[t], there, send_sem.at[t], recv_sem.at[t], **to(2 * chip + p))

    def far(t):
        return lax.rem(lax.div(t, 3), chips) < chips - 1

    def tile(t, _):
        kind, g = lax.rem(t, 3), lax.div(t, 3)
        pair, _, _ = place(g)
        slot = lax.rem(t, RING)
        arrived(slot)
        left = jnp.concatenate([a[n] for n in range(tiles)], 1)
        right = jnp.concatenate([ring[slot, n].reshape(width, TILE) for n in range(WIDE // TILE)], 1)
        y = jnp.dot(left, right, preferred_element_type=jnp.float32)
        table = lax.div(kind, 2)
        for h in range(per):
            u = y[:, h * HEAD : (h + 1) * HEAD].astype(jnp.bfloat16).astype(jnp.float32)
            u = (u * cos[table] + pltpu.roll(u, HEAD // 2, 1) * sin[table]).astype(jnp.bfloat16)
            made[t, h] = u
            got[kind, pair * per + h, pl.ds(pl.multiple_of(c * tokens, tokens), tokens), :] = u

        @pl.when(t + RING < 3 * groups)
        def _():
            fetch(t + RING)

        @pl.when(t + RING >= 3 * groups)
        def _():
            fetch_out(t + RING - 3 * groups)

        @pl.when((t > 0) & far(t + 3 * groups - 1))
        def _():
            parcel(t - 1).start()

    lax.fori_loop(0, 3 * groups, tile, None)

    def residual(n, _):
        rows = pl.ds(pl.multiple_of(n * 16, 16), 16)
        acc[rows, :] = xall[rows, pl.ds(pl.multiple_of(p * half, half), half)].astype(jnp.float32)

    lax.fori_loop(0, tokens // 16, residual, None)

    e = HEAD**-0.5 * LOG2E
    spans = chips * tokens // SPAN
    each = SPAN // tokens

    def ship(pair, chip):
        j = _xor(c, chip, bits)
        return pltpu.make_async_remote_copy(
            outs.at[pair, chip], seen.at[pair * chips + c, p], osend_sem.at[pair, chip], orecv_sem.at[pair, j], **to(2 * chip + p))

    def span_of(m):
        return _xor(lax.div(c, each), _pick(m, SPANS), bits - 1)

    def ship_span(pair, m):
        for n in range(each):
            chip = span_of(m) * each + n

            @pl.when(chip != c)
            def _():
                ship(pair, chip).start()

    def attend(pair, _):
        def take(n, _):
            parcel(pair * 3 * chips + n).wait_recv()

        lax.fori_loop(0, 3 * (chips - 1), take, None)

        def turn(n, _):
            here = pl.ds(pl.multiple_of(n * SPAN, SPAN), SPAN)
            for h in range(per):
                turned_v[h, :HEAD, here] = got[2, pair * per + h, here, :].T
                turned_v[h, HEAD:, here] = jnp.ones((8, SPAN), jnp.bfloat16)

        lax.fori_loop(0, spans, turn, None)

        def span(m, _):
            at = span_of(m)
            mine = pl.ds(pl.multiple_of(at * SPAN, SPAN), SPAN)
            for h in range(per):
                top_s[h] = jnp.full((1, SPAN), NEG, jnp.float32)
                mix_s[h] = jnp.zeros((HEAD + 8, SPAN), jnp.float32)

            def block(j, masked):
                here = pl.ds(pl.multiple_of(j * SPAN, SPAN), SPAN)
                scores = [_dot(got[1, pair * per + h, here, :], got[0, pair * per + h, mine, :], 1, 1) for h in range(per)]
                weights, keeps = [], []
                for h, s in enumerate(scores):
                    if masked:
                        ok = lax.broadcasted_iota(jnp.int32, s.shape, 1) >= lax.broadcasted_iota(jnp.int32, s.shape, 0)
                        s = jnp.where(ok, s, HIDDEN)
                    old = top_s[h]
                    top = jnp.maximum(old, s.max(axis=0, keepdims=True))
                    top_s[h] = top
                    weights.append(jnp.exp2((s - top) * e).astype(jnp.bfloat16))
                    keeps.append(jnp.exp2((old - top) * e))
                for h, (w, keep) in enumerate(zip(weights, keeps)):
                    mix_s[h] = mix_s[h] * keep + _dot(turned_v[h, :, here], w, 1, 0)

            lax.fori_loop(0, at, lambda j, _: block(j, False), None)
            block(at, True)
            for h in range(per):
                out = (mix_s[h, :HEAD, :] * (1 / mix_s[h, HEAD : HEAD + 1, :])).T.astype(jnp.bfloat16)
                for n in range(each):
                    chip = at * each + n
                    piece = out[n * tokens : (n + 1) * tokens]
                    outs[pair, chip, h] = piece
                    seen[jnp.where(chip == c, pair * chips + c, groups), p, h] = piece

            @pl.when(m > 0)
            def _():
                ship_span(pair, m - 1)

        lax.fori_loop(0, spans, span, None)
        ship_span(pair, jnp.int32(spans - 1))

    lax.fori_loop(0, 2, attend, None)

    def hand(s):
        pair, _, chip = block_of(s)
        there = seen.at[pair * chips + chip, p]
        return pltpu.make_async_remote_copy(there, there, dsend_sem.at[s], drecv_sem.at[s], **to(partner))

    def take_in(s):
        pair, j, chip = block_of(s)

        @pl.when(j > 0)
        def _():
            ship(pair, chip).wait_recv()

        hand(s).start()

    take_in(jnp.int32(0))

    def project(s, _):
        pair, _, chip = block_of(s)
        slot = lax.rem(s, RING)

        @pl.when(s + 1 < groups)
        def _():
            take_in(s + 1)

        arrived(slot)
        hand(s).wait_recv()
        left = jnp.concatenate([seen[pair * chips + chip, i, h] for i in range(2) for h in range(per)], 1)
        for n in range(half // WIDE):
            cols = slice(n * WIDE, (n + 1) * WIDE)
            slabs = [divmod(n * (WIDE // TILE) + i, half // WIDE) for i in range(WIDE // TILE)]
            right = jnp.concatenate([ring[slot, i, j].reshape(2 * PART, TILE) for i, j in slabs], 1)
            acc[:, cols] += jnp.dot(left, right, preferred_element_type=jnp.float32)

        @pl.when(s + RING < groups)
        def _():
            fetch_out(s + RING)

    lax.fori_loop(0, groups, project, None)

    parts = 4
    size = half // parts

    def y_copies(n):
        cols = pl.ds(n * size, size)
        there = pl.ds(pl.multiple_of(p * half + n * size, size), size)
        return (pltpu.make_async_copy(xall.at[own_rows, cols], y_hbm.at[:, there], y_sem.at[n]),
                pltpu.make_async_remote_copy(xall.at[other_rows, cols], y_hbm.at[:, there], ysend_sem.at[n], yrecv_sem.at[n], **to(partner)))

    for n in range(parts + 1):
        if n < parts:
            cols = slice(n * size, (n + 1) * size)
            xall[:, cols] = acc[:, cols].astype(jnp.bfloat16)
        if n:
            for copy in y_copies(n - 1):
                copy.start()

    def sent(n, _):
        hand(n).wait_send()

        @pl.when(far(3 * n))
        def _():
            for kind in range(3):
                parcel(3 * n + kind).wait_send()

        pair, chip = lax.div(n, chips), lax.rem(n, chips)

        @pl.when(chip != c)
        def _():
            ship(pair, chip).wait_send()

    lax.fori_loop(0, groups, sent, None)
    for n in range(parts):
        for copy in y_copies(n):
            copy.wait()


def solution(mesh):
    chips = mesh.shape["sp"] // 2

    def step(x, gain, wq, wk, wv, wo):
        own, width = x.shape
        tokens, half, groups = 2 * own, width // 2, 2 * chips
        place = lax.div(lax.axis_index("sp"), 2) * tokens + jnp.arange(tokens)
        angle = place.astype(jnp.float32)[:, None] * THETA ** (-jnp.arange(HEAD // 2, dtype=jnp.float32) / (HEAD // 2))
        cos, sin = jnp.cos(angle), jnp.sin(angle)
        cos, sin = jnp.concatenate([cos, cos], 1), jnp.concatenate([-sin, sin], 1)
        cos, sin = jnp.stack([cos, jnp.ones_like(cos)]), jnp.stack([sin, jnp.zeros_like(sin)])
        per = WIDE // HEAD
        low = jnp.bfloat16
        any_, vmem = pl.BlockSpec(memory_space=pl.ANY), pl.BlockSpec(memory_space=pltpu.VMEM)
        dma = pltpu.SemaphoreType.DMA
        whole = lambda w: w.reshape(width // (2 * PART), 2, PART, width)
        return pl.pallas_call(
            functools.partial(_kernel, chips=chips),
            out_shape=jax.ShapeDtypeStruct((own, width), low),
            in_specs=[any_, vmem, vmem, vmem, any_, any_, any_, any_],
            out_specs=any_,
            scratch_shapes=[
                pltpu.VMEM((tokens, width), low),
                pltpu.VMEM((width // TILE, tokens, TILE), low),
                pltpu.VMEM((RING, WIDE // TILE, width // (2 * PART), 2, PART, TILE), low),
                pltpu.VMEM((3 * groups, per, tokens, HEAD), low),
                pltpu.VMEM((3, 2 * per, chips * tokens, HEAD), low),
                pltpu.VMEM((per, HEAD + 8, chips * tokens), low),
                pltpu.VMEM((2, chips, per, tokens, HEAD), low),
                pltpu.VMEM((groups + 1, 2, per, tokens, HEAD), low),
                pltpu.VMEM((tokens, half), jnp.float32),
                pltpu.VMEM((per, 1, SPAN), jnp.float32),
                pltpu.VMEM((per, HEAD + 8, SPAN), jnp.float32),
                dma((3,)), dma((RING,)), dma((3 * groups,)), dma((3 * groups,)), dma((2, chips)), dma((2, chips)),
                dma((groups,)), dma((groups,)), dma((4,)), dma((4,)), dma((4,)),
            ],
            compiler_params=pltpu.CompilerParams(collective_id=0, has_side_effects=True, vmem_limit_bytes=63 * 2**20),
        )(x, gain[None], cos, sin, whole(wq), whole(wk), whole(wv), wo.reshape(2, half, width))

    tokens, whole = P(("dp", "sp"), None), P(None, None)
    return jax.shard_map(
        step,
        mesh=mesh,
        in_specs=(tokens, P(None), whole, whole, whole, whole),
        out_specs=tokens,
        check_vma=False,
    )
```

```python
import functools

import jax
import jax.numpy as jnp
from jax import lax
from jax.experimental import pallas as pl
from jax.experimental.pallas import tpu as pltpu
from jax.sharding import PartitionSpec as P

HEAD = 128
THETA = 10000
LOG2E = 1.4426950408889634
NEG = -1e30
HIDDEN = 2 * NEG
PART = 256
WIDE = 256
TILE = 128
RING = 6
SPAN = 512
STRIP = 256
SEND = (7, 6, 1, 5, 2, 3, 4, 0)
SPANS = (3, 0, 2, 1)
TAKE = (0, 7, 6, 1, 5, 4, 3, 2)
MESH = pl.DeviceIdType.MESH


def _xor(a, b, bits):
    total = 0
    for n in range(bits):
        w = 2**n
        total += lax.rem(lax.rem(lax.div(a, w), 2) + lax.rem(lax.div(b, w), 2), 2) * w
    return total


def _pick(n, values):
    got = values[-1]
    for i in range(len(values) - 1):
        got = jnp.where(n == i, values[i], got)
    return got


def _dot(a, b, ca, cb):
    return lax.dot_general(a, b, (((ca,), (cb,)), ((), ())), preferred_element_type=jnp.float32)


def _kernel(x_hbm, tables, wq, wk, wv, wo, y_hbm,
            xall, a, ring, raw, turns, made, got, turned_v, outs, seen, acc, top_s, mix_s,
            x_sem, ring_sem, send_sem, recv_sem, osend_sem, orecv_sem, dsend_sem, drecv_sem, ysend_sem, yrecv_sem, y_sem,
            *, chips):
    bits = chips.bit_length() - 1
    own = x_hbm.shape[0]
    tokens = 2 * own
    width = x_hbm.shape[1]
    half = width // 2
    groups = 2 * chips
    per = WIDE // HEAD
    me = lax.axis_index("sp")
    c, p = lax.div(me, 2), lax.rem(me, 2)
    partner = me + 1 - 2 * p

    def to(device):
        return dict(device_id={"sp": device}, device_id_type=MESH)

    barrier = pltpu.get_barrier_semaphore()
    pl.semaphore_signal(barrier, inc=1, **to(partner))
    for j in range(1, chips):
        pl.semaphore_signal(barrier, inc=1, **to(2 * _xor(c, j, bits) + p))

    def first_row(pair, chip):
        return pl.multiple_of((chip * 2 + pair) * WIDE, WIDE)

    def place(g):
        pair, jj = lax.div(g, chips), lax.rem(g, chips)
        return pair, jj, _xor(c, _pick(jj, SEND), bits)

    def fetch(t):
        kind, g = lax.rem(t, 3), lax.div(t, 3)
        pair, _, chip = place(g)
        at = pl.multiple_of(p * half + first_row(pair, chip), WIDE)
        slot = lax.rem(t, RING)
        for k, w in enumerate((wq, wk, wv)):
            @pl.when(kind == k)
            def _():
                for n in range(WIDE // TILE):
                    cols = pl.ds(pl.multiple_of(at + n * TILE, TILE), TILE)
                    pltpu.make_async_copy(w.at[:, :, :, cols], ring.at[slot, n], ring_sem.at[slot]).start()

    def block_of(s):
        pair, jj = lax.div(s, chips), lax.rem(s, chips)
        j = _pick(jj, TAKE)
        return pair, j, _xor(c, j, bits)

    def fetch_out(s):
        pair, _, chip = block_of(s)
        slot = lax.rem(s, RING)
        rows = pl.ds(first_row(pair, chip), WIDE)
        for n in range(half // TILE):
            at = pl.multiple_of(p * half + n * TILE, TILE)
            pltpu.make_async_copy(wo.at[:, rows, pl.ds(at, TILE)], ring.at[slot, *divmod(n, half // WIDE)], ring_sem.at[slot]).start()

    def arrived(slot):
        pltpu.make_async_copy(ring.at[slot], ring.at[slot], ring_sem.at[slot]).wait()

    own_rows = pl.ds(pl.multiple_of(p * own, own), own)
    other_rows = pl.ds(pl.multiple_of((1 - p) * own, own), own)
    local = pltpu.make_async_copy(x_hbm, xall.at[own_rows], x_sem.at[0])
    local.start()
    for t in range(RING):
        fetch(jnp.int32(t))
    pl.semaphore_wait(barrier, chips)
    across = pltpu.make_async_remote_copy(x_hbm, xall.at[own_rows], x_sem.at[1], x_sem.at[2], **to(partner))
    across.start()

    tiles = width // TILE
    band = 32

    def norm(start):
        def rows(n, _):
            at = pl.ds(pl.multiple_of(start + n * band, band), band)
            total = jnp.zeros((band, TILE), jnp.float32)
            for t in range(tiles):
                wide = xall[at, t * TILE : (t + 1) * TILE].astype(jnp.float32)
                total += wide * wide
            scale = lax.rsqrt(jnp.sum(total, -1, keepdims=True) * (1 / width) + 1e-6)
            for t in range(tiles):
                wide = xall[at, t * TILE : (t + 1) * TILE].astype(jnp.float32)
                a[t, at, :] = (wide * scale * tables[2 * tokens + t : 2 * tokens + t + 1, :]).astype(jnp.bfloat16)

        lax.fori_loop(0, own // band, rows, None)

    local.wait()
    norm(p * own)
    across.wait()
    norm((1 - p) * own)

    def parcel(t):
        kind, g = lax.rem(t, 3), lax.div(t, 3)
        pair, _, chip = place(g)
        there = got.at[kind, pl.ds(pair * per, per), pl.ds(pl.multiple_of(c * tokens, tokens), tokens), :]
        return pltpu.make_async_remote_copy(made.at[t], there, send_sem.at[t], recv_sem.at[t], **to(2 * chip + p))

    def far(t):
        return lax.rem(lax.div(t, 3), chips) < chips - 1

    def finish(t):
        kind, g = lax.rem(t, 3), lax.div(t, 3)
        pair, _, _ = place(g)
        table = lax.div(kind, 2)
        for h in range(per):
            u = raw[lax.rem(t, 2), :, h * HEAD : (h + 1) * HEAD].astype(jnp.bfloat16).astype(jnp.float32)
            u = (u * turns[table, 0] + pltpu.roll(u, HEAD // 2, 1) * turns[table, 1]).astype(jnp.bfloat16)
            made[t, h] = u
            got[kind, pair * per + h, pl.ds(pl.multiple_of(c * tokens, tokens), tokens), :] = u

    def tile(t, _):
        slot = lax.rem(t, RING)
        arrived(slot)
        finish(lax.rem(t + 3 * groups - 1, 3 * groups))
        left = jnp.concatenate([a[n] for n in range(tiles)], 1)
        right = jnp.concatenate([ring[slot, n].reshape(width, TILE) for n in range(WIDE // TILE)], 1)
        raw[lax.rem(t, 2)] = jnp.dot(left, right, preferred_element_type=jnp.float32)

        @pl.when(t + RING < 3 * groups)
        def _():
            fetch(t + RING)

        @pl.when(t + RING >= 3 * groups)
        def _():
            fetch_out(t + RING - 3 * groups)

        @pl.when((t > 1) & far(t + 3 * groups - 2))
        def _():
            parcel(t - 2).start()

    turns[0, 0], turns[0, 1] = tables[:tokens, :], tables[tokens : 2 * tokens, :]
    turns[1, 0], turns[1, 1] = jnp.ones((tokens, HEAD), jnp.float32), jnp.zeros((tokens, HEAD), jnp.float32)
    raw[...] = jnp.zeros_like(raw)
    lax.fori_loop(0, 3 * groups, tile, None)
    finish(jnp.int32(3 * groups - 1))

    def residual(n, _):
        rows = pl.ds(pl.multiple_of(n * 16, 16), 16)
        acc[rows, :] = xall[rows, pl.ds(pl.multiple_of(p * half, half), half)].astype(jnp.float32)

    lax.fori_loop(0, tokens // 16, residual, None)

    e = HEAD**-0.5 * LOG2E
    spans = chips * tokens // SPAN
    each = SPAN // tokens

    def ship(pair, chip):
        j = _xor(c, chip, bits)
        return pltpu.make_async_remote_copy(
            outs.at[pair, chip], seen.at[pair * chips + c, p], osend_sem.at[pair, chip], orecv_sem.at[pair, j], **to(2 * chip + p))

    def span_of(m):
        return _xor(lax.div(c, each), _pick(m, SPANS), bits - 1)

    def ship_span(pair, m):
        for n in range(each):
            chip = span_of(m) * each + n

            @pl.when(chip != c)
            def _():
                ship(pair, chip).start()

    def attend(pair, _):
        def take(n, _):
            parcel(pair * 3 * chips + n).wait_recv()

        lax.fori_loop(0, 3 * (chips - 1), take, None)

        def turn(n, _):
            here = pl.ds(pl.multiple_of(n * SPAN, SPAN), SPAN)
            for h in range(per):
                turned_v[h, :HEAD, here] = got[2, pair * per + h, here, :].T
                turned_v[h, HEAD:, here] = jnp.ones((8, SPAN), jnp.bfloat16)

        lax.fori_loop(0, spans, turn, None)

        def span(m, _):
            at = span_of(m)
            for h in range(per):
                top_s[h] = jnp.full((1, SPAN), NEG, jnp.float32)
                mix_s[h] = jnp.zeros((HEAD + 8, SPAN), jnp.float32)

            def block(j, masked):
                here = pl.multiple_of(j * SPAN, SPAN)
                strips = [(h, n) for h in range(per) for n in range(0, SPAN, STRIP)]
                scores = []
                for h, n in strips:
                    keys = n + STRIP if masked else SPAN
                    scores.append(_dot(got[1, pair * per + h, pl.ds(here, keys), :],
                                       got[0, pair * per + h, pl.ds(pl.multiple_of(at * SPAN + n, STRIP), STRIP), :], 1, 1))
                weights, keeps = [], []
                for (h, n), s in zip(strips, scores):
                    cols = slice(n, n + STRIP)
                    if masked:
                        ok = lax.broadcasted_iota(jnp.int32, s.shape, 1) + n >= lax.broadcasted_iota(jnp.int32, s.shape, 0)
                        s = jnp.where(ok, s, HIDDEN)
                    old = top_s[h, :, cols]
                    top = jnp.maximum(old, s.max(axis=0, keepdims=True))
                    top_s[h, :, cols] = top
                    weights.append(jnp.exp2((s - top) * e).astype(jnp.bfloat16))
                    keeps.append(jnp.exp2((old - top) * e))
                for (h, n), w, keep in zip(strips, weights, keeps):
                    cols = slice(n, n + STRIP)
                    mix_s[h, :, cols] = mix_s[h, :, cols] * keep + _dot(turned_v[h, :, pl.ds(here, w.shape[0])], w, 1, 0)

            lax.fori_loop(0, at, lambda j, _: block(j, False), None)
            block(at, True)
            for h in range(per):
                out = (mix_s[h, :HEAD, :] * (1 / mix_s[h, HEAD : HEAD + 1, :])).T.astype(jnp.bfloat16)
                for n in range(each):
                    chip = at * each + n
                    piece = out[n * tokens : (n + 1) * tokens]
                    outs[pair, chip, h] = piece
                    seen[jnp.where(chip == c, pair * chips + c, groups), p, h] = piece

            @pl.when(m > 0)
            def _():
                ship_span(pair, m - 1)

        lax.fori_loop(0, spans, span, None)
        ship_span(pair, jnp.int32(spans - 1))

    lax.fori_loop(0, 2, attend, None)

    def hand(s):
        pair, _, chip = block_of(s)
        there = seen.at[pair * chips + chip, p]
        return pltpu.make_async_remote_copy(there, there, dsend_sem.at[s], drecv_sem.at[s], **to(partner))

    def take_in(s):
        pair, j, chip = block_of(s)

        @pl.when(j > 0)
        def _():
            ship(pair, chip).wait_recv()

        hand(s).start()

    take_in(jnp.int32(0))

    def project(s, _):
        pair, _, chip = block_of(s)
        slot = lax.rem(s, RING)

        @pl.when(s + 1 < groups)
        def _():
            take_in(s + 1)

        arrived(slot)
        hand(s).wait_recv()
        left = jnp.concatenate([seen[pair * chips + chip, i, h] for i in range(2) for h in range(per)], 1)
        for n in range(half // WIDE):
            cols = slice(n * WIDE, (n + 1) * WIDE)
            slabs = [divmod(n * (WIDE // TILE) + i, half // WIDE) for i in range(WIDE // TILE)]
            right = jnp.concatenate([ring[slot, i, j].reshape(2 * PART, TILE) for i, j in slabs], 1)
            acc[:, cols] += jnp.dot(left, right, preferred_element_type=jnp.float32)

        @pl.when(s + RING < groups)
        def _():
            fetch_out(s + RING)

    lax.fori_loop(0, groups, project, None)

    parts = 4
    size = half // parts

    def y_copies(n):
        cols = pl.ds(n * size, size)
        there = pl.ds(pl.multiple_of(p * half + n * size, size), size)
        return (pltpu.make_async_copy(xall.at[own_rows, cols], y_hbm.at[:, there], y_sem.at[n]),
                pltpu.make_async_remote_copy(xall.at[other_rows, cols], y_hbm.at[:, there], ysend_sem.at[n], yrecv_sem.at[n], **to(partner)))

    for n in range(parts + 1):
        if n < parts:
            cols = slice(n * size, (n + 1) * size)
            xall[:, cols] = acc[:, cols].astype(jnp.bfloat16)
        if n:
            for copy in y_copies(n - 1):
                copy.start()

    def sent(n, _):
        hand(n).wait_send()

        @pl.when(far(3 * n))
        def _():
            for kind in range(3):
                parcel(3 * n + kind).wait_send()

        pair, chip = lax.div(n, chips), lax.rem(n, chips)

        @pl.when(chip != c)
        def _():
            ship(pair, chip).wait_send()

    lax.fori_loop(0, groups, sent, None)
    for n in range(parts):
        for copy in y_copies(n):
            copy.wait()


def solution(mesh):
    chips = mesh.shape["sp"] // 2

    def step(x, gain, wq, wk, wv, wo):
        own, width = x.shape
        tokens, half, groups = 2 * own, width // 2, 2 * chips
        place = lax.div(lax.axis_index("sp"), 2) * tokens + jnp.arange(tokens)
        angle = place.astype(jnp.float32)[:, None] * THETA ** (-jnp.arange(HEAD // 2, dtype=jnp.float32) / (HEAD // 2))
        cos, sin = jnp.cos(angle), jnp.sin(angle)
        cos, sin = jnp.concatenate([cos, cos], 1), jnp.concatenate([-sin, sin], 1)
        tables = jnp.concatenate([cos, sin, gain.reshape(-1, TILE).astype(jnp.float32)])
        per = WIDE // HEAD
        low = jnp.bfloat16
        any_, vmem = pl.BlockSpec(memory_space=pl.ANY), pl.BlockSpec(memory_space=pltpu.VMEM)
        dma = pltpu.SemaphoreType.DMA
        whole = lambda w: w.reshape(width // (2 * PART), 2, PART, width)
        return pl.pallas_call(
            functools.partial(_kernel, chips=chips),
            out_shape=jax.ShapeDtypeStruct((own, width), low),
            in_specs=[any_, vmem, any_, any_, any_, any_],
            out_specs=any_,
            scratch_shapes=[
                pltpu.VMEM((tokens, width), low),
                pltpu.VMEM((width // TILE, tokens, TILE), low),
                pltpu.VMEM((RING, WIDE // TILE, width // (2 * PART), 2, PART, TILE), low),
                pltpu.VMEM((2, tokens, WIDE), jnp.float32),
                pltpu.VMEM((2, 2, tokens, HEAD), jnp.float32),
                pltpu.VMEM((3 * groups, per, tokens, HEAD), low),
                pltpu.VMEM((3, 2 * per, chips * tokens, HEAD), low),
                pltpu.VMEM((per, HEAD + 8, chips * tokens), low),
                pltpu.VMEM((2, chips, per, tokens, HEAD), low),
                pltpu.VMEM((groups + 1, 2, per, tokens, HEAD), low),
                pltpu.VMEM((tokens, half), jnp.float32),
                pltpu.VMEM((per, 1, SPAN), jnp.float32),
                pltpu.VMEM((per, HEAD + 8, SPAN), jnp.float32),
                dma((3,)), dma((RING,)), dma((3 * groups,)), dma((3 * groups,)), dma((2, chips)), dma((2, chips)),
                dma((groups,)), dma((groups,)), dma((4,)), dma((4,)), dma((4,)),
            ],
            compiler_params=pltpu.CompilerParams(collective_id=0, has_side_effects=True, vmem_limit_bytes=63 * 2**20),
        )(x, tables, whole(wq), whole(wk), whole(wv), wo.reshape(2, half, width))

    tokens, whole = P(("dp", "sp"), None), P(None, None)
    return jax.shard_map(
        step,
        mesh=mesh,
        in_specs=(tokens, P(None), whole, whole, whole, whole),
        out_specs=tokens,
        check_vma=False,
    )
```
